256 devices in a mesh: groups: 2 (over z), ep: 128 (over y, x, core).
Axes of the slice: x: 8, y: 8, z: 2, core: 2. Of those that a mesh axis runs over, the one named last changes fastest.
The devices are a block of a 8x8x16 slice.
Arguments:
- tokens: bfloat16 [2048, 7168], P(('groups', 'ep')), parts along dimension 0, may hold values from -6 to 6
- experts: int32 [2048, 8], P(('groups', 'ep')), parts along dimension 0, may hold values from 0 to 15, as said below
- gate_fixed: int32 [2048, 8], P(('groups', 'ep')), parts along dimension 0, may hold values from 1 to 65535
- home_slot: int32 [2048], P(('groups', 'ep')), parts along dimension 0, may hold values from 0 to 7, as said below
- bias: float32 [16], replicated, may hold values from -0.5 to 0.5
- w_gate: bfloat16 [7168, 32768], P(None, 'ep'), may hold values from -0.0625 to 0.0625
- w_up: bfloat16 [7168, 32768], P(None, 'ep'), may hold values from -0.0625 to 0.0625
- w_down: bfloat16 [32768, 7168], P('ep'), may hold values from -0.125 to 0.125
Outputs:
- moe_out: bfloat16 [2048, 7168], P(('groups', 'ep')), parts along dimension 0
- bias_next: float32 [32], P('groups'), parts along dimension 0
The draws below stay inside these ranges and needn't reach their ends.
There are 2 independent parts, one for each index of `groups`. The reference program is written for one: setup_inputs(seed, part) draws one part's arguments, and reference() takes and returns one part's arrays. A program takes and returns all parts, laid end to end along the dimension named above; an argument that names none is the same for every part. Nothing has to cross between parts.
Inputs may be any that keep to these rules, and one draw needn't show every extreme that they name: Each token names 8 different experts; among the tokens of one device no expert is named more than 6 times, and some device reaches that bound. `home_slot`: within each device's block of 8 tokens every value appears exactly once.
All inputs are finite; a program needn't handle non-finite values.
Results may differ from the reference program's by a relative error of at most 0.008.
Values may be sent and summed in bfloat16 or wider, within the bound.
A program may use at most 128 MiB of HBM per device.

```python
import math
import jax
import jax.numpy as jnp
from jax import lax

D = 7168
FF = 2048
TOP = 8
EXPERTS = 16
TOK_DEV = 8
SHARDS = 8
FF_DEV = 256
TOKENS = 1024
CAP = 6
N_EP = 128


def draw_home_slot(key, part):
    block_count = TOKENS // TOK_DEV
    scores = jax.random.randint(key, (block_count, TOK_DEV), 0, 1 << 20, dtype=jnp.int32)
    scores = scores * TOK_DEV + jnp.arange(TOK_DEV, dtype=jnp.int32)[None, :]
    ordering = jnp.argsort(scores, axis=1, stable=True).astype(jnp.int32)
    return ordering.reshape(TOKENS)


def draw_experts(key, part):
    block_count = TOKENS // TOK_DEV
    pair_count = TOK_DEV * TOP
    narrow = min(EXPERTS, max(TOP, -(-pair_count // CAP)))
    base = jax.random.fold_in(key, 17)
    first_key = jax.random.fold_in(base, 1)
    second_key = jax.random.fold_in(base, 2)
    third_key = jax.random.fold_in(base, 3)
    common_scores = jax.random.randint(first_key, (EXPERTS,), 0, 1 << 20, dtype=jnp.int32)
    common_scores = common_scores * EXPERTS + jnp.arange(EXPERTS, dtype=jnp.int32)
    common = jnp.argsort(common_scores, stable=True).astype(jnp.int32)
    block_scores = jax.random.randint(second_key, (block_count, EXPERTS), 0, 1 << 20, dtype=jnp.int32)
    block_scores = block_scores * EXPERTS + jnp.arange(EXPERTS, dtype=jnp.int32)[None, :]
    block_order = jnp.argsort(block_scores, axis=1, stable=True).astype(jnp.int32)
    coin = jax.random.randint(third_key, (block_count,), 0, max(block_count - 1, 1), dtype=jnp.int32)
    concentrated = coin < jnp.arange(block_count, dtype=jnp.int32)
    pair_index = jnp.arange(pair_count, dtype=jnp.int32)
    hot_ids = common[pair_index % narrow]
    spread_index = jnp.broadcast_to((pair_index % EXPERTS)[None, :], (block_count, pair_count))
    spread_ids = jnp.take_along_axis(block_order, spread_index, axis=1)
    chosen = jnp.where(concentrated[:, None], hot_ids[None, :], spread_ids)
    return chosen.reshape(TOKENS, TOP).astype(jnp.int32)


def plant(values, rng, least, high):
    place = [jax.random.randint(jax.random.fold_in(rng, axis), (), 0, length) for axis, length in enumerate(values.shape)]
    longest = values.shape.index(max(values.shape))
    neighbour = place[:longest] + [(place[longest] + 1) % values.shape[longest]] + place[longest + 1:]
    return values.at[tuple(place)].set(least).at[tuple(neighbour)].set(high)


def block_levels(stream_key, shape, cuts, smallest, largest):
    def one(dim, blocks):
        draws = jax.random.uniform(jax.random.fold_in(jax.random.fold_in(stream_key, 6), dim), (blocks,), jnp.float32, smallest / len(cuts), largest / len(cuts))
        return jnp.repeat(jnp.exp(draws), shape[dim] // blocks).reshape((-1,) + (1,) * (len(shape) - dim - 1))

    factor_of = one(*cuts[0])
    for cut in cuts[1:]:
        factor_of = factor_of * one(*cut)
    return factor_of


def normal_values(stream_key, extent, deviation, reach, split=(), kind=jnp.bfloat16):
    factor_of = block_levels(stream_key, extent, split, -0.22, 0.18) if split else 1.0
    result = jax.random.normal(stream_key, extent, jnp.float32) * deviation * factor_of
    return jnp.minimum(jnp.maximum(result, -reach), reach).astype(kind)


def setup_inputs(seed: int = 0, part: int = 0) -> dict:
    key_list = jax.random.split(jax.random.key(seed), 9)
    part_keys = jax.random.split(jax.random.fold_in(key_list[8], part), 9)
    tokens = normal_values(part_keys[0], (TOKENS, D), 1.0, 6.0, ((0, 128),))
    experts = draw_experts(jax.random.fold_in(jax.random.fold_in(key_list[8], part), 71), part)
    gate_fixed = plant(jax.random.randint(part_keys[2], (TOKENS, TOP), 1, 65536), jax.random.fold_in(part_keys[2], 1), 1, 65535).astype(jnp.int32)
    home_slot = draw_home_slot(jax.random.fold_in(jax.random.fold_in(key_list[8], part), 71), part)
    bias = jnp.clip(jax.random.uniform(key_list[4], (EXPERTS,), jnp.float32, -0.5, 0.5), -0.5, 0.5)
    w_gate = normal_values(key_list[5], (D, EXPERTS * FF), D ** -0.5, 0.0625, ((1, 128),))
    w_up = normal_values(key_list[6], (D, EXPERTS * FF), D ** -0.5, 0.0625, ((1, 128),))
    w_down = normal_values(key_list[7], (EXPERTS * FF, D), FF ** -0.5, 0.125, ((0, 128),))
    return dict(tokens=tokens, experts=experts, gate_fixed=gate_fixed, home_slot=home_slot, bias=bias, w_gate=w_gate, w_up=w_up, w_down=w_down)


ROUTED_SCALE = 2.5

def reference(tokens, experts, gate_fixed, home_slot, bias, w_gate, w_up, w_down):
    pair_count = TOK_DEV * TOP
    flat_ids = experts.reshape(N_EP, pair_count)
    hit_table = (flat_ids[:, :, None] == jnp.arange(EXPERTS, dtype=jnp.int32)[None, None, :]).astype(jnp.int32)
    earlier = jnp.cumsum(hit_table, axis=1) - hit_table
    slot_rank = lax.optimization_barrier(jnp.sum(earlier * hit_table, axis=2)).astype(jnp.int32)
    pair_token = jnp.arange(N_EP, dtype=jnp.int32)[:, None] * TOK_DEV + jnp.arange(pair_count, dtype=jnp.int32)[None, :] // TOP
    position = ((jnp.arange(N_EP, dtype=jnp.int32)[:, None] * EXPERTS + flat_ids) * CAP + slot_rank).reshape(-1)
    fixed_gate = gate_fixed.astype(jnp.float32)
    gate_share = ROUTED_SCALE * fixed_gate / lax.optimization_barrier(jnp.sum(fixed_gate, axis=1, keepdims=True))
    source_table = jnp.full((N_EP * EXPERTS * CAP,), -1, jnp.int32).at[position].set(pair_token.reshape(-1))
    source_table = source_table.reshape(N_EP, EXPERTS, CAP)
    share_table = jnp.zeros((N_EP * EXPERTS * CAP,), jnp.float32).at[position].set(gate_share.reshape(-1))
    share_table = share_table.reshape(N_EP, EXPERTS, CAP)

    def one_expert(running, expert_id):
        index_rows = lax.dynamic_index_in_dim(source_table, expert_id, 1, keepdims=False).reshape(-1)
        share_rows = lax.dynamic_index_in_dim(share_table, expert_id, 1, keepdims=False).reshape(-1)
        valid = index_rows >= 0
        safe_rows = jnp.maximum(index_rows, 0)
        row_block = jnp.where(valid[:, None], tokens[safe_rows], jnp.zeros((), jnp.bfloat16))
        first = (expert_id * FF).astype(jnp.int32)
        gate_cols = lax.dynamic_slice_in_dim(w_gate, first, FF, 1)
        up_cols = lax.dynamic_slice_in_dim(w_up, first, FF, 1)
        down_rows = lax.dynamic_slice_in_dim(w_down, first, FF, 0)
        gate_part = jnp.dot(row_block, gate_cols, preferred_element_type=jnp.float32)
        up_part = jnp.dot(row_block, up_cols, preferred_element_type=jnp.float32)
        hidden = (jax.nn.silu(gate_part) * up_part).astype(jnp.bfloat16)
        row_count = hidden.shape[0]
        hidden_groups = hidden.astype(jnp.float32).reshape(row_count, SHARDS, FF_DEV)
        down_groups = down_rows.astype(jnp.float32).reshape(SHARDS, FF_DEV, D)
        partial_value = jnp.einsum('rsf,sfd->rsd', hidden_groups, down_groups).astype(jnp.bfloat16)
        expert_out = lax.optimization_barrier(jnp.sum(partial_value.astype(jnp.float32), axis=1))
        weighted = jnp.where(valid[:, None], expert_out * share_rows[:, None], jnp.zeros((), jnp.float32))
        return (running.at[safe_rows].add(weighted), None)
    start = jnp.zeros((N_EP * TOK_DEV, D), jnp.float32)
    summed, _ = lax.scan(one_expert, start, jnp.arange(EXPERTS, dtype=jnp.int32))
    combined = summed.astype(jnp.bfloat16).reshape(N_EP, TOK_DEV, D)
    block_ids = jnp.broadcast_to(jnp.arange(N_EP, dtype=jnp.int32)[:, None], (N_EP, TOK_DEV))
    placed = jnp.zeros((N_EP, TOK_DEV, D), jnp.bfloat16).at[block_ids, home_slot.reshape(N_EP, TOK_DEV)].set(combined)
    moe_out = placed.reshape(N_EP * TOK_DEV, D)
    load = lax.optimization_barrier(jnp.sum(hit_table, axis=(0, 1))).astype(jnp.float32)
    average = N_EP * TOK_DEV * TOP / EXPERTS
    bias_next = bias + 2.0 / math.sqrt(average) * (average - load)
    return (moe_out, bias_next)
```

```python
import math

import jax
import jax.numpy as jnp
from jax import lax
from jax.sharding import PartitionSpec as P

ROUTED_SCALE = 2.5


def per_device(tokens, experts, gate_fixed, home_slot, bias, w_gate, w_up, w_down):
    tok_rows, width = tokens.shape
    top_count = experts.shape[1]
    expert_count = bias.shape[0]
    device_count = lax.axis_size("ep")
    shards = device_count // expert_count
    meta = jnp.concatenate([experts, gate_fixed // 256, gate_fixed % 256], axis=1)
    rows = jnp.concatenate([tokens, meta.astype(jnp.bfloat16)], axis=1)
    placer = (home_slot[None, :] == jnp.arange(tok_rows, dtype=jnp.int32)[:, None]).astype(jnp.bfloat16)
    rows = jnp.dot(placer, rows, preferred_element_type=jnp.float32).astype(jnp.bfloat16)
    everyone = lax.all_gather(rows, "ep", axis=0, tiled=True)
    x = everyone[:, :width]
    meta = everyone[:, width:].astype(jnp.float32)
    ids, high, low = meta[:, :top_count], meta[:, top_count : 2 * top_count], meta[:, 2 * top_count :]
    fixed = high * 256.0 + low
    share = ROUTED_SCALE * fixed / jnp.sum(fixed, axis=1, keepdims=True)
    own = (lax.axis_index("ep") // shards).astype(jnp.float32)
    gate = jnp.sum(jnp.where(ids == own, share, 0.0), axis=1, keepdims=True)
    gate_part = jnp.dot(x, w_gate, preferred_element_type=jnp.float32)
    up_part = jnp.dot(x, w_up, preferred_element_type=jnp.float32)
    hidden = (jax.nn.silu(gate_part) * up_part * gate).astype(jnp.bfloat16)
    part = jnp.dot(hidden, w_down, preferred_element_type=jnp.float32).astype(jnp.bfloat16)
    out = lax.psum_scatter(part, "ep", scatter_dimension=0, tiled=True)
    hits = ids[:, :, None] == jnp.arange(expert_count, dtype=jnp.float32)[None, None, :]
    loads = jnp.sum(hits.astype(jnp.float32), axis=(0, 1))
    average = tok_rows * device_count * top_count / expert_count
    bias_next = bias + 2.0 / math.sqrt(average) * (average - loads)
    return (out, bias_next)


def solution(mesh):
    placed = (
        P(("groups", "ep"), None),
        P(("groups", "ep"), None),
        P(("groups", "ep"), None),
        P(("groups", "ep")),
        P(),
        P(None, "ep"),
        P(None, "ep"),
        P("ep", None),
    )
    return jax.shard_map(
        per_device,
        mesh=mesh,
        in_specs=placed,
        out_specs=(P(("groups", "ep"), None), P("groups")),
        check_vma=False,
    )
```

```python
import functools
import math

import jax
import jax.numpy as jnp
from jax import lax
from jax.experimental import pallas as pl
from jax.experimental.pallas import tpu as pltpu
from jax.sharding import PartitionSpec as P

ROUTED_SCALE = 2.5
F32 = jnp.float32
BF16 = jnp.bfloat16


def when(cond):
    return pl.when(cond)


def kernel(
    dims, home, tok, exp_ref, gate_ref, bias_ref, wg, wu, wd,
    out, bias_out,
    xs, xr, x_own, x_par, wgu, wdn, acc, hid, pst, prx, ring, z_out, z_in, fin, f_out, f_in,
    w_sem, x_sem, s1, r1, s2, r2, sd, rd, sp, rp, sr, rr, sz, rz, sf,
):
    side, experts, shards, average = dims
    R, H = side, side // 2
    top = exp_ref.shape[1]
    half = tok.shape[1] // 2
    wide = half + 128
    cut = (half // 2) // 128 * 128
    ff = wg.shape[1]
    me = lax.axis_index("ep")
    core = me % 2
    x = (me // 2) % side
    y = me // (2 * side)
    a = y + core * (x - y)
    b = x + core * (y - x)

    def device(aa, bb):
        yy = aa + core * (bb - aa)
        xx = bb + core * (aa - bb)
        return {"ep": (yy * side + xx) * 2 + core}

    a_next, a_prev = device((a + 1) % R, b), device((a + R - 1) % R, b)
    b_next, b_prev = device(a, (b + 1) % R), device(a, (b + R - 1) % R)
    partner = {"ep": me + 1 - 2 * core}
    b_to = (b_next, b_prev)

    def remote(src, dst, send, recv, to):
        return pltpu.make_async_remote_copy(
            src_ref=src, dst_ref=dst, send_sem=send, recv_sem=recv,
            device_id=to, device_id_type=pl.DeviceIdType.MESH,
        )

    weights = []
    for h in range(2):
        rows = pl.ds(h * half, half)
        weights.append(pltpu.make_async_copy(wg.at[rows, :], wgu.at[h, :, pl.ds(0, ff)], w_sem.at[3 * h]))
        weights.append(pltpu.make_async_copy(wu.at[rows, :], wgu.at[h, :, pl.ds(ff, ff)], w_sem.at[3 * h + 1]))
        weights.append(pltpu.make_async_copy(wd.at[:, rows], wdn.at[h], w_sem.at[3 * h + 2]))
    for w in weights:
        w.start()

    barrier = pltpu.get_barrier_semaphore()
    for to in (partner, a_next, a_prev, b_next, b_prev):
        pl.semaphore_signal(barrier, inc=1, device_id=to, device_id_type=pl.DeviceIdType.MESH)

    fixed = gate_ref[...].astype(F32)
    share = ROUTED_SCALE * fixed / jnp.sum(fixed, axis=1, keepdims=True)
    ids = exp_ref[...]
    lane = lax.broadcasted_iota(jnp.int32, (tok.shape[0], 128), 1)
    expert_of = lane % experts
    hit = jnp.zeros(lane.shape, F32)
    val = jnp.zeros(lane.shape, F32)
    for k in range(top):
        same = expert_of == ids[:, k : k + 1]
        hit = hit + jnp.where(same, 1.0, 0.0)
        val = val + jnp.where(same, share[:, k : k + 1], 0.0)
    high = val.astype(BF16).astype(F32)
    rest = val - high
    mid = rest.astype(BF16).astype(F32)
    low = rest - mid
    part = lane // experts
    meta = jnp.where(part == 0, hit, 0.0)
    meta = jnp.where(part == 1, high, meta)
    meta = jnp.where(part == 2, mid, meta)
    meta = jnp.where(part == 3, low, meta)
    first = core == 0
    lo_half = tok[:, pl.ds(0, half)].astype(F32)
    hi_half = tok[:, pl.ds(half, half)].astype(F32)
    mine = jnp.where(first, lo_half, hi_half)
    xs[:, pl.ds(0, half)] = jnp.where(first, hi_half, lo_half).astype(BF16)
    xs[:, pl.ds(half, 128)] = meta.astype(BF16)

    pl.semaphore_wait(barrier, 5)
    swap = remote(xs, xr, x_sem.at[0], x_sem.at[1], partner)
    swap.start()
    swap.wait_recv()
    got = xr[...].astype(F32)
    x_own[0, 0, :, pl.ds(0, half)] = jnp.where(
        first,
        jnp.concatenate([mine, got[:, :half]], axis=0),
        jnp.concatenate([got[:, :half], mine], axis=0),
    ).astype(BF16)
    x_own[0, 0, :, pl.ds(half, 128)] = jnp.where(
        first,
        jnp.concatenate([meta, got[:, half:]], axis=0),
        jnp.concatenate([got[:, half:], meta], axis=0),
    ).astype(BF16)

    def down(g):
        src = jnp.maximum(2 * g - 1, 0) if not isinstance(g, int) else max(2 * g - 1, 0)
        return remote(x_own.at[0, src], x_own.at[0, 2 * g + 1], s1.at[1, g], r1.at[1, g], a_prev)

    def up(g):
        return remote(x_own.at[0, 2 * g], x_own.at[0, 2 * g + 2], s1.at[0, g], r1.at[0, g], a_next)

    down(0).start()
    up(0).start()

    def clear(j, c):
        for d in range(2):
            ring[d, H, j] = jnp.zeros((16, half), BF16)
        ring[0, H - 1, j, :, pl.ds(cut, half - cut)] = jnp.zeros((16, half - cut), BF16)
        ring[1, H - 1, j, :, pl.ds(0, cut)] = jnp.zeros((16, cut), BF16)
        acc[j] = jnp.zeros(acc.shape[1:], F32)
        return c

    lax.fori_loop(0, R, clear, 0)
    for d in range(2):
        z_in[d, H] = jnp.zeros((16, half), BF16)

    whole = pl.ds(0, wide)
    lows, highs = pl.ds(0, cut), pl.ds(cut, wide - cut)

    def ring_x(d, s, g, cols):
        n = s if d == 0 else (R - s) % R
        to = s + 1 if d == 0 else R - s - 1
        return remote(
            x_own.at[n, pl.ds(2 * g, 2), :, cols], x_own.at[to, pl.ds(2 * g, 2), :, cols],
            s2.at[d, s, g], r2.at[d, s, g], b_to[d],
        )

    def across(n, g):
        return remote(
            x_own.at[n, pl.ds(2 * g, 2)], x_par.at[n, pl.ds(2 * g, 2)], sd.at[n, g], rd.at[n, g], partner
        )

    def gather_step(k, g):
        s = k - g

        @when(s == 0)
        def _():
            down(g).wait_recv()

            @when(g < H - 1)
            def _():
                down(g + 1).start()
                up(g).wait_recv()

            @when(g < H - 2)
            def _():
                up(g + 1).start()

        @when((s >= 1) & (s < H))
        def _():
            for d in range(2):
                ring_x(d, s - 1, g, whole).wait_recv()

        @when(s == H)
        def _():
            ring_x(0, H - 1, g, lows).wait_recv()
            ring_x(1, H - 1, g, highs).wait_recv()

        @when((s >= 0) & (s < H - 1))
        def _():
            for d in range(2):
                ring_x(d, s, g, whole).start()

        @when(s == H - 1)
        def _():
            ring_x(0, H - 1, g, lows).start()
            ring_x(1, H - 1, g, highs).start()

        @when((s >= 0) & (s <= H))
        def _():
            across(s, g).start()

        @when((s >= 1) & (s < H))
        def _():
            across(R - s, g).start()

    def own_block(n):
        rows = x_own[n, :, :, pl.ds(0, half)].reshape(R * 16, half)
        prod = jnp.dot(rows, wgu[core], preferred_element_type=F32)
        acc[n] += prod.reshape(R, 16, 2 * ff)

    def slot_of(n):
        return jnp.where(n < H, 2 * n, 2 * R - 1 - 2 * n)

    def par_block(n):
        for g in range(H):
            across(n, g).wait_recv()
        rows = x_par[n, :, :, pl.ds(0, half)].reshape(R * 16, half)
        prod = jnp.dot(rows, wgu[1 - core], preferred_element_type=F32)
        j = slot_of(n)
        for t in range(R):
            m = t // 2 if t % 2 == 0 else R - 1 - t // 2
            acc[m, j] += prod[16 * t : 16 * t + 16]

    def gather_stage(k, c):
        lax.fori_loop(0, H, lambda g, cc: (gather_step(k, g), cc)[1], 0)

        @when(k == H - 1)
        def _():
            for w in weights:
                w.wait()

        @when(k >= H - 1)
        def _():
            s = k - (H - 1)
            count = jnp.where((s >= 1) & (s < H), 2, 1)

            def own(i, cc):
                own_block(s + i * (R - 2 * s))
                return cc

            def par(i, cc):
                par_block(s + i * (R - 2 * s))
                return cc

            lax.fori_loop(0, count, own, 0)
            lax.fori_loop(0, count, par, 0)

        return c

    lax.fori_loop(0, 2 * H, gather_stage, 0)

    my_expert = me // shards
    lane = lax.broadcasted_iota(jnp.int32, (R * 16, 128), 1)
    gated = (lane % experts == my_expert) & (lane >= experts) & (lane < 4 * experts)

    def activate(n, total):
        m = x_own[n, :, :, pl.ds(half, 128)].reshape(R * 16, 128).astype(F32)
        gate = jnp.sum(jnp.where(gated, m, 0.0), axis=1, keepdims=True)
        both = acc[n].reshape(R * 16, 2 * ff)
        v = both[:, :ff]
        h = v / (1.0 + jnp.exp(-v)) * both[:, ff:] * gate
        hid[n] = h.astype(BF16).reshape(R, 16, ff)
        return total + jnp.sum(m, axis=0, keepdims=True)

    loads = lax.fori_loop(0, R, activate, jnp.zeros((1, 128), F32))
    bias_out[...] = bias_ref[...] + 2.0 / math.sqrt(average) * (average - loads[:, :experts])

    C = 512 if half % 512 == 0 else 128

    def to_partner(g, s):
        return remote(pst.at[g, s], prx.at[g, s], sp.at[g, s], rp.at[g, s], partner)

    def partner_chunk(g, s):
        j1, j2 = slot_of((R - s) % R), slot_of(s)
        lhs = jnp.concatenate(
            [hid[g, j1], hid[R - 1 - g, j1], hid[g, j2], hid[R - 1 - g, j2]], axis=0
        )

        def cols(t, cc):
            at = pl.ds(pl.multiple_of(t * C, 128), C)
            p = jnp.dot(lhs, wdn[1 - core, :, at], preferred_element_type=F32)
            pst[g, s, :, :, :, at] = p.astype(BF16).reshape(2, 2, 16, C)
            return cc

        lax.fori_loop(0, half // C, cols, 0)
        to_partner(g, s).start()

    whole_z = pl.ds(0, half)
    lows_z, highs_z = pl.ds(0, cut), pl.ds(cut, half - cut)

    def ring_r(d, s, g, cols):
        return remote(
            ring.at[d, s, pl.ds(2 * g, 2), :, cols], ring.at[d, s - 1, pl.ds(2 * g, 2), :, cols],
            sr.at[d, s - 1, g], rr.at[d, s - 1, g], b_to[d],
        )

    def z_up(g):
        return remote(z_out.at[0, g], z_in.at[0, g], sz.at[0, g], rz.at[0, g], a_next)

    def z_down(g):
        return remote(z_out.at[1, g], z_in.at[1, g], sz.at[1, g], rz.at[1, g], a_prev)

    def own_chunk(g, s):
        to_partner(g, s).wait_recv()

        @when(s < H - 1)
        def _():
            for d in range(2):
                ring_r(d, s + 1, g, whole_z).wait_recv()

        @when(s == H - 1)
        def _():
            ring_r(0, H, g, lows_z).wait_recv()
            ring_r(1, H, g, highs_z).wait_recv()

        pair = pl.ds(2 * g, 2)

        @when(s >= 1)
        def _():
            lhs = jnp.concatenate(
                [hid[(R - s) % R, pair].reshape(32, ff), hid[s, pair].reshape(32, ff)], axis=0
            )

            def cols(t, cc):
                at = pl.ds(pl.multiple_of(t * C, 128), C)
                p = jnp.dot(lhs, wdn[core, :, at], preferred_element_type=F32).reshape(2, 2, 16, C)
                p = p + prx[g, s, :, :, :, at].astype(F32)
                for d in range(2):
                    ring[d, s, pair, :, at] = (p[d] + ring[d, s, pair, :, at].astype(F32)).astype(BF16)
                return cc

            lax.fori_loop(0, half // C, cols, 0)

            @when(s < H)
            def _():
                for d in range(2):
                    ring_r(d, s, g, whole_z).start()

            @when(s == H)
            def _():
                ring_r(0, H, g, lows_z).start()
                ring_r(1, H, g, highs_z).start()

        @when(s == 0)
        def _():
            @when(g < H - 1)
            def _():
                z_up(g + 1).wait_recv()
                z_down(g + 1).wait_recv()

            lhs = hid[0, pair].reshape(32, ff)

            def cols(t, cc):
                at = pl.ds(pl.multiple_of(t * C, 128), C)
                p = jnp.dot(lhs, wdn[core, :, at], preferred_element_type=F32).reshape(2, 16, C)
                p = p + prx[g, 0, 0, :, :, at].astype(F32)
                p = p + ring[0, 0, pair, :, at].astype(F32) + ring[1, 0, pair, :, at].astype(F32)
                near = p[0] + z_in[1, g + 1, :, at].astype(F32)
                far = p[1] + z_in[0, g + 1, :, at].astype(F32)
                fin[:, at] = near
                z_out[1, g, :, at] = near.astype(BF16)
                z_out[0, g, :, at] = far.astype(BF16)
                return cc

            lax.fori_loop(0, half // C, cols, 0)
            z_up(g).start()

            @when(g >= 1)
            def _():
                z_down(g).start()

    def sum_stage(k, c):
        def own(i, cc):
            s = H - (k - 1) + i

            @when((s >= 0) & (s <= H) & (k >= 1))
            def _():
                own_chunk(H - 1 - i, s)

            return cc

        def other(i, cc):
            s = H - k + i

            @when((s >= 0) & (s <= H))
            def _():
                partner_chunk(H - 1 - i, s)

            return cc

        lax.fori_loop(0, H, own, 0)
        lax.fori_loop(0, H, other, 0)
        return c

    lax.fori_loop(0, 2 * H + 1, sum_stage, 0)
    z_up(0).wait_recv()

    total = fin[...] + z_in[0, 0].astype(F32)
    f_out[...] = jnp.where(first, total[8:], total[:8])
    kept = jnp.where(first, total[:8], total[8:])
    last = remote(f_out, f_in, sf.at[0], sf.at[1], partner)
    last.start()
    row = lax.broadcasted_iota(jnp.int32, (8, half), 0)

    def place(v):
        v = v.astype(BF16).astype(F32)
        placed = jnp.zeros((8, half), F32)
        for t in range(8):
            placed = jnp.where(row == home[t], jnp.broadcast_to(v[t : t + 1], (8, half)), placed)
        return placed

    kept = place(kept)

    swap.wait_send()

    def drain_g(g, c):
        down(g).wait_send()

        @when(g < H - 1)
        def _():
            up(g).wait_send()

        def per_s(s, cc):
            @when(s < H - 1)
            def _():
                for d in range(2):
                    ring_x(d, s, g, whole).wait_send()

            @when(s == H - 1)
            def _():
                ring_x(0, H - 1, g, lows).wait_send()
                ring_x(1, H - 1, g, highs).wait_send()
                ring_r(0, H, g, lows_z).wait_send()
                ring_r(1, H, g, highs_z).wait_send()

            @when(s < H - 1)
            def _():
                for d in range(2):
                    ring_r(d, s + 1, g, whole_z).wait_send()

            return cc

        lax.fori_loop(0, H, per_s, 0)

        def per_n(n, cc):
            across(n, g).wait_send()
            return cc

        lax.fori_loop(0, R, per_n, 0)

        def per_p(s, cc):
            to_partner(g, s).wait_send()
            return cc

        lax.fori_loop(0, H + 1, per_p, 0)
        z_up(g).wait_send()

        @when(g >= 1)
        def _():
            z_down(g).wait_send()

        return c

    lax.fori_loop(0, H, drain_g, 0)

    last.wait()
    other = place(f_in[...])
    out[:, pl.ds(0, half)] = jnp.where(first, kept, other).astype(BF16)
    out[:, pl.ds(half, half)] = jnp.where(first, other, kept).astype(BF16)


def per_device(tokens, experts, gate_fixed, home_slot, bias, w_gate, w_up, w_down):
    tok_rows, width = tokens.shape
    count = bias.shape[0]
    devices = lax.axis_size("ep")
    shards = devices // count
    side = math.isqrt(devices // 2)
    R, H = side, side // 2
    half = width // 2
    ff = w_gate.shape[1]
    average = tok_rows * devices * experts.shape[1] / count
    vmem = pl.BlockSpec(memory_space=pltpu.VMEM)
    smem = pl.BlockSpec(memory_space=pltpu.SMEM)
    anywhere = pl.BlockSpec(memory_space=pl.ANY)
    dma = pltpu.SemaphoreType.DMA
    out, bias_next = pl.pallas_call(
        functools.partial(kernel, (side, count, shards, average)),
        out_shape=(
            jax.ShapeDtypeStruct((tok_rows, width), BF16),
            jax.ShapeDtypeStruct((1, count), F32),
        ),
        in_specs=[smem, vmem, vmem, vmem, vmem, anywhere, anywhere, anywhere],
        out_specs=(vmem, vmem),
        scratch_shapes=[
            pltpu.VMEM((tok_rows, half + 128), BF16),
            pltpu.VMEM((tok_rows, half + 128), BF16),
            pltpu.VMEM((R, R, 16, half + 128), BF16),
            pltpu.VMEM((R, R, 16, half + 128), BF16),
            pltpu.VMEM((2, half, 2 * ff), BF16),
            pltpu.VMEM((2, ff, half), BF16),
            pltpu.VMEM((R, R, 16, 2 * ff), F32),
            pltpu.VMEM((R, R, 16, ff), BF16),
            pltpu.VMEM((H, H + 1, 2, 2, 16, half), BF16),
            pltpu.VMEM((H, H + 1, 2, 2, 16, half), BF16),
            pltpu.VMEM((2, H + 1, R, 16, half), BF16),
            pltpu.VMEM((2, H, 16, half), BF16),
            pltpu.VMEM((2, H + 1, 16, half), BF16),
            pltpu.VMEM((16, half), F32),
            pltpu.VMEM((tok_rows, half), F32),
            pltpu.VMEM((tok_rows, half), F32),
            dma((6,)),
            dma((2,)),
            dma((2, H)),
            dma((2, H)),
            dma((2, H, H)),
            dma((2, H, H)),
            dma((R, H)),
            dma((R, H)),
            dma((H, H + 1)),
            dma((H, H + 1)),
            dma((2, H, H)),
            dma((2, H, H)),
            dma((2, H)),
            dma((2, H)),
            dma((2,)),
        ],
        compiler_params=pltpu.CompilerParams(
            collective_id=0, has_side_effects=True, vmem_limit_bytes=67_000_000
        ),
        name="routed_experts",
    )(home_slot, tokens, experts, gate_fixed, bias.reshape(1, count), w_gate, w_up, w_down)
    return (out, bias_next.reshape(count))


def solution(mesh):
    placed = (
        P(("groups", "ep"), None),
        P(("groups", "ep"), None),
        P(("groups", "ep"), None),
        P(("groups", "ep")),
        P(),
        P(None, "ep"),
        P(None, "ep"),
        P("ep", None),
    )
    return jax.shard_map(
        per_device,
        mesh=mesh,
        in_specs=placed,
        out_specs=(P(("groups", "ep"), None), P("groups")),
        check_vma=False,
    )
```

```python
import functools
import math

import jax
import jax.numpy as jnp
from jax import lax
from jax.experimental import pallas as pl
from jax.experimental.pallas import tpu as pltpu
from jax.sharding import PartitionSpec as P

ROUTED_SCALE = 2.5
F32 = jnp.float32
BF16 = jnp.bfloat16


def when(cond):
    return pl.when(cond)


def kernel(
    dims, home, tok, exp_ref, gate_ref, bias_ref, wg, wu, wd,
    out, bias_out,
    xs, xr, x_own, x_par, wgu, wdn, acc_own, acc_par, hid, pst, prx, ring, z_out, z_in, fin, f_out, f_in, loads,
    w_sem, x_sem, s1, r1, s2, r2, sd, rd, sp, rp, sr, rr, sz, rz, sf,
):
    side, experts, shards, average = dims
    R, H = side, side // 2
    top = exp_ref.shape[1]
    half = tok.shape[1] // 2
    wide = half + 128
    cut = (half // 2) // 128 * 128
    ff = wg.shape[1]
    me = lax.axis_index("ep")
    core = me % 2
    x = (me // 2) % side
    y = me // (2 * side)
    a = y + core * (x - y)
    b = x + core * (y - x)

    def device(aa, bb):
        yy = aa + core * (bb - aa)
        xx = bb + core * (aa - bb)
        return {"ep": (yy * side + xx) * 2 + core}

    a_next, a_prev = device((a + 1) % R, b), device((a + R - 1) % R, b)
    b_next, b_prev = device(a, (b + 1) % R), device(a, (b + R - 1) % R)
    partner = {"ep": me + 1 - 2 * core}
    b_to = (b_next, b_prev)

    def remote(src, dst, send, recv, to):
        return pltpu.make_async_remote_copy(
            src_ref=src, dst_ref=dst, send_sem=send, recv_sem=recv,
            device_id=to, device_id_type=pl.DeviceIdType.MESH,
        )

    weights = []
    for h in range(2):
        rows = pl.ds(h * half, half)
        weights.append(pltpu.make_async_copy(wg.at[rows, :], wgu.at[h, :, pl.ds(0, ff)], w_sem.at[3 * h]))
        weights.append(pltpu.make_async_copy(wu.at[rows, :], wgu.at[h, :, pl.ds(ff, ff)], w_sem.at[3 * h + 1]))
        weights.append(pltpu.make_async_copy(wd.at[:, rows], wdn.at[h], w_sem.at[3 * h + 2]))
    for w in weights:
        w.start()

    barrier = pltpu.get_barrier_semaphore()
    for to in [partner, b_next, b_prev] + [device((a + i) % R, b) for i in range(1, R)]:
        pl.semaphore_signal(barrier, inc=1, device_id=to, device_id_type=pl.DeviceIdType.MESH)

    fixed = gate_ref[...].astype(F32)
    share = ROUTED_SCALE * fixed / jnp.sum(fixed, axis=1, keepdims=True)
    ids = exp_ref[...]
    lane = lax.broadcasted_iota(jnp.int32, (tok.shape[0], 128), 1)
    expert_of = lane % experts
    hit = jnp.zeros(lane.shape, F32)
    val = jnp.zeros(lane.shape, F32)
    for k in range(top):
        same = expert_of == ids[:, k : k + 1]
        hit = hit + jnp.where(same, 1.0, 0.0)
        val = val + jnp.where(same, share[:, k : k + 1], 0.0)
    high = val.astype(BF16).astype(F32)
    rest = val - high
    mid = rest.astype(BF16).astype(F32)
    low = rest - mid
    part = lane // experts
    meta = jnp.where(part == 0, hit, 0.0)
    meta = jnp.where(part == 1, high, meta)
    meta = jnp.where(part == 2, mid, meta)
    meta = jnp.where(part == 3, low, meta)
    first = core == 0
    lo_half = tok[:, pl.ds(0, half)].astype(F32)
    hi_half = tok[:, pl.ds(half, half)].astype(F32)
    mine = jnp.where(first, lo_half, hi_half)
    xs[:, pl.ds(0, half)] = jnp.where(first, hi_half, lo_half).astype(BF16)
    xs[:, pl.ds(half, 128)] = meta.astype(BF16)

    pl.semaphore_wait(barrier, R + 2)
    swap = remote(xs, xr, x_sem.at[0], x_sem.at[1], partner)
    swap.start()
    swap.wait_recv()
    got = xr[...].astype(F32)
    x_own[0, 0, :, pl.ds(0, half)] = jnp.where(
        first,
        jnp.concatenate([mine, got[:, :half]], axis=0),
        jnp.concatenate([got[:, :half], mine], axis=0),
    ).astype(BF16)
    x_own[0, 0, :, pl.ds(half, 128)] = jnp.where(
        first,
        jnp.concatenate([meta, got[:, half:]], axis=0),
        jnp.concatenate([got[:, half:], meta], axis=0),
    ).astype(BF16)

    def down(g):
        src = jnp.maximum(2 * g - 1, 0) if not isinstance(g, int) else max(2 * g - 1, 0)
        return remote(x_own.at[0, src], x_own.at[0, 2 * g + 1], s1.at[1, g], r1.at[1, g], a_prev)

    def up(g):
        return remote(x_own.at[0, 2 * g], x_own.at[0, 2 * g + 2], s1.at[0, g], r1.at[0, g], a_next)

    down(0).start()
    up(0).start()

    def clear(j, c):
        ring[0, H - 1, j, :, pl.ds(cut, half - cut)] = jnp.zeros((16, half - cut), BF16)
        ring[1, H - 1, j, :, pl.ds(0, cut)] = jnp.zeros((16, cut), BF16)
        return c

    lax.fori_loop(0, R, clear, 0)

    whole = pl.ds(0, wide)
    lows, highs = pl.ds(0, cut), pl.ds(cut, wide - cut)

    def ring_x(d, s, g, cols):
        n = s if d == 0 else (R - s) % R
        to = s + 1 if d == 0 else R - s - 1
        return remote(
            x_own.at[n, pl.ds(2 * g, 2), :, cols], x_own.at[to, pl.ds(2 * g, 2), :, cols],
            s2.at[d, s, g], r2.at[d, s, g], b_to[d],
        )

    def across(n, g):
        return remote(
            x_own.at[n, pl.ds(2 * g, 2)], x_par.at[n, pl.ds(2 * g, 2)], sd.at[n, g], rd.at[n, g], partner
        )

    def gather_step(k, g):
        s = k - g

        @when(s == 0)
        def _():
            down(g).wait_recv()

            @when(g < H - 1)
            def _():
                down(g + 1).start()
                up(g).wait_recv()

            @when(g < H - 2)
            def _():
                up(g + 1).start()

        @when((s >= 1) & (s < H))
        def _():
            for d in range(2):
                ring_x(d, s - 1, g, whole).wait_recv()

        @when(s == H)
        def _():
            ring_x(0, H - 1, g, lows).wait_recv()
            ring_x(1, H - 1, g, highs).wait_recv()

        @when((s >= 0) & (s < H - 1))
        def _():
            for d in range(2):
                ring_x(d, s, g, whole).start()

        @when(s == H - 1)
        def _():
            ring_x(0, H - 1, g, lows).start()
            ring_x(1, H - 1, g, highs).start()

        @when((s >= 0) & (s <= H))
        def _():
            across(s, g).start()

        @when((s >= 1) & (s < H))
        def _():
            across(R - s, g).start()

    def slot_of(n):
        return jnp.where(n < H, 2 * n, 2 * R - 1 - 2 * n)

    def pair(g):
        return pl.ds(2 * g, 2)

    def gate_up(x_ref, acc_ref, w, chunks):
        at = [(n, pair(g)) for g, s in chunks for n in (s, (R - s) % R)]
        rows = jnp.concatenate(
            [x_ref[n, p, :, pl.ds(0, half)].reshape(32, half) for n, p in at], axis=0
        )
        prod = jnp.dot(rows, wgu[w], preferred_element_type=F32)
        for i, (n, p) in enumerate(at):
            acc_ref[n, p] = prod[32 * i : 32 * i + 32].reshape(2, 16, 2 * ff)

    def arrivals(k, body):
        def unit(u, c):
            s0 = k - 2 * u
            v0 = (s0 >= 0) & (s0 <= H)
            v1 = (s0 >= 1) & (s0 <= H + 1)

            @when(v0 | v1)
            def _():
                g0 = 2 * u + jnp.where(v0, 0, 1)
                g1 = 2 * u + jnp.where(v1, 1, 0)
                body(v0, v1, [(g0, k - g0), (g1, k - g1)])

            return c

        lax.fori_loop(0, H // 2, unit, 0)

    def own_arrivals(v0, v1, chunks):
        gate_up(x_own, acc_own, core, chunks)

    def par_arrivals(v0, v1, chunks):
        for v, (g, s) in zip((v0, v1), chunks):
            @when(v)
            def _(g=g, s=s):
                across(s, g).wait_recv()

                @when((s >= 1) & (s < H))
                def _():
                    across(R - s, g).wait_recv()

        gate_up(x_par, acc_par, 1 - core, chunks)

    my_expert = me // shards
    lane = lax.broadcasted_iota(jnp.int32, (32, 128), 1)
    gated = (lane % experts == my_expert) & (lane >= experts) & (lane < 4 * experts)

    def activate(n, g):
        m = x_own[n, pair(g), :, pl.ds(half, 128)].reshape(32, 128).astype(F32)
        gate = jnp.sum(jnp.where(gated, m, 0.0), axis=1, keepdims=True)
        j = slot_of(n)
        both = acc_own[n, pair(g)].reshape(32, 2 * ff) + jnp.concatenate(
            [acc_par[g, j], acc_par[R - 1 - g, j]], axis=0
        )
        v = both[:, :ff]
        h = v / (1.0 + jnp.exp(-v)) * both[:, ff:] * gate
        hid[n, pair(g)] = h.astype(BF16).reshape(2, 16, ff)
        loads[...] += jnp.sum(m, axis=0, keepdims=True)

    loads[...] = jnp.zeros((1, 128), F32)

    C = 512 if half % 512 == 0 else 128

    def to_partner(g, s):
        return remote(pst.at[g, s], prx.at[g, s], sp.at[g, s], rp.at[g, s], partner)

    def partner_chunk(g, s):
        j1, j2 = slot_of((R - s) % R), slot_of(s)
        lhs = jnp.concatenate(
            [hid[g, j1], hid[R - 1 - g, j1], hid[g, j2], hid[R - 1 - g, j2]], axis=0
        )

        def cols(t, cc):
            at = pl.ds(t * C, C)
            p = jnp.dot(lhs, wdn[1 - core, :, at], preferred_element_type=F32)
            pst[g, s, :, :, :, at] = p.astype(BF16).reshape(2, 2, 16, C)
            return cc

        for t in range(half // C):
            cols(t, 0)
        to_partner(g, s).start()

    def own_chunk(g, s):
        lhs = jnp.concatenate(
            [hid[(R - s) % R, pair(g)].reshape(32, ff), hid[s, pair(g)].reshape(32, ff)], axis=0
        )
        to_partner(g, s).wait_recv()

        def cols(t, cc):
            at = pl.ds(t * C, C)
            p = jnp.dot(lhs, wdn[core, :, at], preferred_element_type=F32).reshape(2, 2, 16, C)
            prx[g, s, :, :, :, at] = (p + prx[g, s, :, :, :, at].astype(F32)).astype(BF16)
            return cc

        for t in range(half // C):
            cols(t, 0)

    whole_z = pl.ds(0, half)
    lows_z, highs_z = pl.ds(0, cut), pl.ds(cut, half - cut)

    def ring_first(d, g):
        cols = highs_z if d else lows_z
        return remote(
            prx.at[g, H, d, :, :, cols], ring.at[d, H - 1, pair(g), :, cols],
            sr.at[d, H - 1, g], rr.at[d, H - 1, g], b_to[d],
        )

    def ring_r(d, s, g):
        return remote(
            ring.at[d, s, pair(g)], ring.at[d, s - 1, pair(g)],
            sr.at[d, s - 1, g], rr.at[d, s - 1, g], b_to[d],
        )

    def z_send(j, to):
        return remote(z_out.at[j], z_in.at[j], sz.at[j], rz.at[j], device(to % R, b))

    def sum_step(k, g):
        s = 2 * H + 1 - k + g

        @when(s == H)
        def _():
            for d in range(2):
                ring_first(d, g).start()

        @when((s >= 0) & (s < H))
        def _():
            for d in range(2):
                @when(s == H - 1)
                def _(d=d):
                    ring_first(d, g).wait_recv()

                @when(s < H - 1)
                def _(d=d):
                    ring_r(d, s + 1, g).wait_recv()

                @when(s >= 1)
                def _(d=d):
                    ring[d, s, pair(g)] = (
                        ring[d, s, pair(g)].astype(F32) + prx[g, s, d].astype(F32)
                    ).astype(BF16)
                    ring_r(d, s, g).start()

        @when(s == 0)
        def _():
            v = ring[0, 0, pair(g)].astype(F32) + ring[1, 0, pair(g)].astype(F32)
            v = v + prx[g, 0, 0].astype(F32)
            z_out[pair(g)] = v.astype(BF16)

            @when(g == 0)
            def _():
                fin[...] = v[0]

            @when(g >= 1)
            def _():
                z_send(2 * g, a + R - g).start()

            z_send(2 * g + 1, a + g + 1).start()

    def over_groups(body):
        lax.fori_loop(0, H, lambda g, c: (body(g), c)[1], 0)

    def stage(k, c):
        over_groups(lambda g: gather_step(k, g))
        over_groups(lambda i: sum_step(k, H - 1 - i))

        @when(k == 0)
        def _():
            for w in weights:
                w.wait()

        arrivals(k, own_arrivals)
        arrivals(k, par_arrivals)
        new = k - H

        @when((new >= 0) & (new < H))
        def _():
            def near(n, cc):
                activate(n, new)
                return cc

            def rest(g, cc):
                activate(new, g)
                activate(R - 1 - new, g)
                return cc

            lax.fori_loop(new, R - new, near, 0)
            lax.fori_loop(new + 1, H, rest, 0)
            partner_chunk(new, H)

        def ahead(g):
            s = H - (k - H - g)

            @when((s >= 1) & (s <= H))
            def _():
                partner_chunk(g, s - 1)

        def base(g):
            s = H - (k - H - g)

            @when((s >= 0) & (s <= H))
            def _():
                own_chunk(g, s)

        over_groups(ahead)
        over_groups(base)
        return c

    lax.fori_loop(0, 3 * H + 1, stage, 0)
    bias_out[...] = bias_ref[...] + 2.0 / math.sqrt(average) * (average - loads[:, pl.ds(0, experts)])

    total = fin[...]
    for j in range(1, R):
        z_send(j, a + 1).wait_recv()
        total = total + z_in[j].astype(F32)
    f_out[...] = jnp.where(first, total[8:], total[:8])
    kept = jnp.where(first, total[:8], total[8:])
    last = remote(f_out, f_in, sf.at[0], sf.at[1], partner)
    last.start()
    row = lax.broadcasted_iota(jnp.int32, (8, half), 0)

    def place(v):
        v = v.astype(BF16).astype(F32)
        placed = jnp.zeros((8, half), F32)
        for t in range(8):
            placed = jnp.where(row == home[t], jnp.broadcast_to(v[t : t + 1], (8, half)), placed)
        return placed

    kept = place(kept)

    swap.wait_send()

    def drain_g(g, c):
        down(g).wait_send()

        @when(g < H - 1)
        def _():
            up(g).wait_send()

        def per_s(s, cc):
            @when(s < H - 1)
            def _():
                for d in range(2):
                    ring_x(d, s, g, whole).wait_send()

            @when(s == H - 1)
            def _():
                ring_x(0, H - 1, g, lows).wait_send()
                ring_x(1, H - 1, g, highs).wait_send()
                for d in range(2):
                    ring_first(d, g).wait_send()

            @when(s < H - 1)
            def _():
                for d in range(2):
                    ring_r(d, s + 1, g).wait_send()

            return cc

        lax.fori_loop(0, H, per_s, 0)

        def per_n(n, cc):
            across(n, g).wait_send()
            return cc

        lax.fori_loop(0, R, per_n, 0)

        def per_p(s, cc):
            to_partner(g, s).wait_send()
            return cc

        lax.fori_loop(0, H + 1, per_p, 0)
        z_send(2 * g + 1, a + 1).wait_send()

        @when(g >= 1)
        def _():
            z_send(2 * g, a + 1).wait_send()

        return c

    lax.fori_loop(0, H, drain_g, 0)

    last.wait()
    other = place(f_in[...])
    out[:, pl.ds(0, half)] = jnp.where(first, kept, other).astype(BF16)
    out[:, pl.ds(half, half)] = jnp.where(first, other, kept).astype(BF16)


def per_device(tokens, experts, gate_fixed, home_slot, bias, w_gate, w_up, w_down):
    tok_rows, width = tokens.shape
    count = bias.shape[0]
    devices = lax.axis_size("ep")
    shards = devices // count
    side = math.isqrt(devices // 2)
    R, H = side, side // 2
    half = width // 2
    ff = w_gate.shape[1]
    average = tok_rows * devices * experts.shape[1] / count
    vmem = pl.BlockSpec(memory_space=pltpu.VMEM)
    smem = pl.BlockSpec(memory_space=pltpu.SMEM)
    anywhere = pl.BlockSpec(memory_space=pl.ANY)
    dma = pltpu.SemaphoreType.DMA
    out, bias_next = pl.pallas_call(
        functools.partial(kernel, (side, count, shards, average)),
        out_shape=(
            jax.ShapeDtypeStruct((tok_rows, width), BF16),
            jax.ShapeDtypeStruct((1, count), F32),
        ),
        in_specs=[smem, vmem, vmem, vmem, vmem, anywhere, anywhere, anywhere],
        out_specs=(vmem, vmem),
        scratch_shapes=[
            pltpu.VMEM((tok_rows, half + 128), BF16),
            pltpu.VMEM((tok_rows, half + 128), BF16),
            pltpu.VMEM((R, R, 16, half + 128), BF16),
            pltpu.VMEM((R, R, 16, half + 128), BF16),
            pltpu.VMEM((2, half, 2 * ff), BF16),
            pltpu.VMEM((2, ff, half), BF16),
            pltpu.VMEM((R, R, 16, 2 * ff), F32),
            pltpu.VMEM((R, R, 16, 2 * ff), F32),
            pltpu.VMEM((R, R, 16, ff), BF16),
            pltpu.VMEM((H, H + 1, 2, 2, 16, half), BF16),
            pltpu.VMEM((H, H + 1, 2, 2, 16, half), BF16),
            pltpu.VMEM((2, H, R, 16, half), BF16),
            pltpu.VMEM((R, 16, half), BF16),
            pltpu.VMEM((R, 16, half), BF16),
            pltpu.VMEM((16, half), F32),
            pltpu.VMEM((tok_rows, half), F32),
            pltpu.VMEM((tok_rows, half), F32),
            pltpu.VMEM((1, 128), F32),
            dma((6,)),
            dma((2,)),
            dma((2, H)),
            dma((2, H)),
            dma((2, H, H)),
            dma((2, H, H)),
            dma((R, H)),
            dma((R, H)),
            dma((H, H + 1)),
            dma((H, H + 1)),
            dma((2, H, H)),
            dma((2, H, H)),
            dma((R,)),
            dma((R,)),
            dma((2,)),
        ],
        compiler_params=pltpu.CompilerParams(
            collective_id=0, has_side_effects=True, vmem_limit_bytes=67_000_000
        ),
        name="routed_experts",
    )(home_slot, tokens, experts, gate_fixed, bias.reshape(1, count), w_gate, w_up, w_down)
    return (out, bias_next.reshape(count))


def solution(mesh):
    placed = (
        P(("groups", "ep"), None),
        P(("groups", "ep"), None),
        P(("groups", "ep"), None),
        P(("groups", "ep")),
        P(),
        P(None, "ep"),
        P(None, "ep"),
        P("ep", None),
    )
    return jax.shard_map(
        per_device,
        mesh=mesh,
        in_specs=placed,
        out_specs=(P(("groups", "ep"), None), P("groups")),
        check_vma=False,
    )
```

```python
import functools
import math

import jax
import jax.numpy as jnp
from jax import lax
from jax.experimental import pallas as pl
from jax.experimental.pallas import tpu as pltpu
from jax.sharding import PartitionSpec as P

ROUTED_SCALE = 2.5
F32 = jnp.float32
BF16 = jnp.bfloat16


def when(cond):
    return pl.when(cond)


def kernel(
    dims, home, tok, exp_ref, gate_ref, bias_ref, wg, wu, wd,
    out, bias_out,
    xs, xr, x_own, x_par, wgu, wdn, acc_own, acc_par, hid, pst, prx, ring, z_out, z_in, fin, f_out, f_in, loads,
    w_sem, x_sem, s1, r1, s2, r2, sd, rd, sp, rp, sr, rr, sz, rz, sf,
):
    side, experts, shards, average = dims
    R, H = side, side // 2
    assert R == 8
    top = exp_ref.shape[1]
    half = tok.shape[1] // 2
    wide = half + 128
    cut = (half // 2) // 128 * 128
    ff = wg.shape[1]
    me = lax.axis_index("ep")
    core = me % 2
    x = (me // 2) % side
    y = me // (2 * side)
    a = y + core * (x - y)
    b = x + core * (y - x)

    def device(aa, bb):
        yy = aa + core * (bb - aa)
        xx = bb + core * (aa - bb)
        return {"ep": (yy * side + xx) * 2 + core}

    a_next, a_prev = device((a + 1) % R, b), device((a + R - 1) % R, b)
    b_next, b_prev = device(a, (b + 1) % R), device(a, (b + R - 1) % R)
    partner = {"ep": me + 1 - 2 * core}
    b_to = (b_next, b_prev)

    def remote(src, dst, send, recv, to):
        return pltpu.make_async_remote_copy(
            src_ref=src, dst_ref=dst, send_sem=send, recv_sem=recv,
            device_id=to, device_id_type=pl.DeviceIdType.MESH,
        )

    weights = []
    for h in range(2):
        rows = pl.ds(h * half, half)
        weights.append(pltpu.make_async_copy(wg.at[rows, :], wgu.at[h, :, pl.ds(0, ff)], w_sem.at[3 * h]))
        weights.append(pltpu.make_async_copy(wu.at[rows, :], wgu.at[h, :, pl.ds(ff, ff)], w_sem.at[3 * h + 1]))
        weights.append(pltpu.make_async_copy(wd.at[:, rows], wdn.at[h], w_sem.at[3 * h + 2]))
    for w in weights:
        w.start()

    barrier = pltpu.get_barrier_semaphore()
    for to in [partner, b_next, b_prev] + [device((a + i) % R, b) for i in (1, 2, R - 2, R - 1)]:
        pl.semaphore_signal(barrier, inc=1, device_id=to, device_id_type=pl.DeviceIdType.MESH)

    fixed = gate_ref[...].astype(F32)
    share = ROUTED_SCALE * fixed / jnp.sum(fixed, axis=1, keepdims=True)
    ids = exp_ref[...]
    lane = lax.broadcasted_iota(jnp.int32, (tok.shape[0], 128), 1)
    expert_of = lane % experts
    hit = jnp.zeros(lane.shape, F32)
    val = jnp.zeros(lane.shape, F32)
    for k in range(top):
        same = expert_of == ids[:, k : k + 1]
        hit = hit + jnp.where(same, 1.0, 0.0)
        val = val + jnp.where(same, share[:, k : k + 1], 0.0)
    high = val.astype(BF16).astype(F32)
    rest = val - high
    mid = rest.astype(BF16).astype(F32)
    low = rest - mid
    part = lane // experts
    meta = jnp.where(part == 0, hit, 0.0)
    meta = jnp.where(part == 1, high, meta)
    meta = jnp.where(part == 2, mid, meta)
    meta = jnp.where(part == 3, low, meta)
    first = core == 0
    lo_half = tok[:, pl.ds(0, half)].astype(F32)
    hi_half = tok[:, pl.ds(half, half)].astype(F32)
    mine = jnp.where(first, lo_half, hi_half)
    xs[:, pl.ds(0, half)] = jnp.where(first, hi_half, lo_half).astype(BF16)
    xs[:, pl.ds(half, 128)] = meta.astype(BF16)

    pl.semaphore_wait(barrier, 7)
    swap = remote(xs, xr, x_sem.at[0], x_sem.at[1], partner)
    swap.start()
    swap.wait_recv()
    got = xr[...].astype(F32)
    x_own[0, 0, :, pl.ds(0, half)] = jnp.where(
        first,
        jnp.concatenate([mine, got[:, :half]], axis=0),
        jnp.concatenate([got[:, :half], mine], axis=0),
    ).astype(BF16)
    x_own[0, 0, :, pl.ds(half, 128)] = jnp.where(
        first,
        jnp.concatenate([meta, got[:, half:]], axis=0),
        jnp.concatenate([got[:, half:], meta], axis=0),
    ).astype(BF16)

    def down(g):
        src = jnp.maximum(2 * g - 1, 0) if not isinstance(g, int) else max(2 * g - 1, 0)
        return remote(x_own.at[0, src], x_own.at[0, 2 * g + 1], s1.at[1, g], r1.at[1, g], a_prev)

    def up(g):
        return remote(x_own.at[0, 2 * g], x_own.at[0, 2 * g + 2], s1.at[0, g], r1.at[0, g], a_next)

    down(0).start()
    up(0).start()

    def clear(j, c):
        ring[0, H - 1, j, :, pl.ds(cut, half - cut)] = jnp.zeros((16, half - cut), BF16)
        ring[1, H - 1, j, :, pl.ds(0, cut)] = jnp.zeros((16, cut), BF16)
        return c

    lax.fori_loop(0, R, clear, 0)

    whole = pl.ds(0, wide)
    lows, highs = pl.ds(0, cut), pl.ds(cut, wide - cut)

    def ring_x(d, s, g, cols):
        n = s if d == 0 else (R - s) % R
        to = s + 1 if d == 0 else R - s - 1
        return remote(
            x_own.at[n, pl.ds(2 * g, 2), :, cols], x_own.at[to, pl.ds(2 * g, 2), :, cols],
            s2.at[d, s, g], r2.at[d, s, g], b_to[d],
        )

    def across(n, g):
        return remote(
            x_own.at[n, pl.ds(2 * g, 2)], x_par.at[n, pl.ds(2 * g, 2)], sd.at[n, g], rd.at[n, g], partner
        )

    def gather_step(k, g):
        s = k - g

        @when(s == 0)
        def _():
            down(g).wait_recv()

            @when(g < H - 1)
            def _():
                down(g + 1).start()
                up(g).wait_recv()

            @when(g < H - 2)
            def _():
                up(g + 1).start()

        @when((s >= 1) & (s < H))
        def _():
            for d in range(2):
                ring_x(d, s - 1, g, whole).wait_recv()

        @when(s == H)
        def _():
            ring_x(0, H - 1, g, lows).wait_recv()
            ring_x(1, H - 1, g, highs).wait_recv()

        @when((s >= 0) & (s < H - 1))
        def _():
            for d in range(2):
                ring_x(d, s, g, whole).start()

        @when(s == H - 1)
        def _():
            ring_x(0, H - 1, g, lows).start()
            ring_x(1, H - 1, g, highs).start()

        @when((s >= 0) & (s <= H))
        def _():
            across(s, g).start()

        @when((s >= 1) & (s < H))
        def _():
            across(R - s, g).start()

    def slot_of(n):
        return jnp.where(n < H, 2 * n, 2 * R - 1 - 2 * n)

    def pair(g):
        return pl.ds(2 * g, 2)

    def gate_up(x_ref, acc_ref, w, chunks):
        at = [(n, pair(g)) for g, s in chunks for n in (s, (R - s) % R)]
        rows = jnp.concatenate(
            [x_ref[n, p, :, pl.ds(0, half)].reshape(32, half) for n, p in at], axis=0
        )
        prod = jnp.dot(rows, wgu[w], preferred_element_type=F32)
        for i, (n, p) in enumerate(at):
            acc_ref[n, p] = prod[32 * i : 32 * i + 32].reshape(2, 16, 2 * ff)

    def arrivals(k, body):
        def unit(u, c):
            s0 = k - 2 * u
            v0 = (s0 >= 0) & (s0 <= H)
            v1 = (s0 >= 1) & (s0 <= H + 1)

            @when(v0 | v1)
            def _():
                g0 = 2 * u + jnp.where(v0, 0, 1)
                g1 = 2 * u + jnp.where(v1, 1, 0)
                body(v0, v1, [(g0, k - g0), (g1, k - g1)])

            return c

        lax.fori_loop(0, H // 2, unit, 0)

    def own_arrivals(v0, v1, chunks):
        gate_up(x_own, acc_own, core, chunks)

    def par_arrivals(v0, v1, chunks):
        for v, (g, s) in zip((v0, v1), chunks):
            @when(v)
            def _(g=g, s=s):
                across(s, g).wait_recv()

                @when((s >= 1) & (s < H))
                def _():
                    across(R - s, g).wait_recv()

        gate_up(x_par, acc_par, 1 - core, chunks)

    my_expert = me // shards
    lane = lax.broadcasted_iota(jnp.int32, (32, 128), 1)
    gated = (lane % experts == my_expert) & (lane >= experts) & (lane < 4 * experts)

    def activate(n, g):
        m = x_own[n, pair(g), :, pl.ds(half, 128)].reshape(32, 128).astype(F32)
        gate = jnp.sum(jnp.where(gated, m, 0.0), axis=1, keepdims=True)
        j = slot_of(n)
        both = acc_own[n, pair(g)].reshape(32, 2 * ff) + jnp.concatenate(
            [acc_par[g, j], acc_par[R - 1 - g, j]], axis=0
        )
        v = both[:, :ff]
        h = v / (1.0 + jnp.exp(-v)) * both[:, ff:] * gate
        hid[n, pair(g)] = h.astype(BF16).reshape(2, 16, ff)
        loads[...] += jnp.sum(m, axis=0, keepdims=True)

    loads[...] = jnp.zeros((1, 128), F32)

    C = 512 if half % 512 == 0 else 128

    def to_partner(g, s):
        return remote(pst.at[g, s], prx.at[g, s], sp.at[g, s], rp.at[g, s], partner)

    def partner_chunks(chunks):
        lhs = []
        for g, s in chunks:
            j1, j2 = slot_of((R - s) % R), slot_of(s)
            lhs += [hid[g, j1], hid[R - 1 - g, j1], hid[g, j2], hid[R - 1 - g, j2]]
        lhs = jnp.concatenate(lhs, axis=0)
        for t in range(half // C):
            at = pl.ds(t * C, C)
            p = jnp.dot(lhs, wdn[1 - core, :, at], preferred_element_type=F32).astype(BF16)
            for i, (g, s) in enumerate(chunks):
                pst[g, s, :, :, :, at] = p[64 * i : 64 * i + 64].reshape(2, 2, 16, C)
        for g, s in chunks:
            to_partner(g, s).start()

    def own_chunks(chunks):
        lhs = []
        for g, s in chunks:
            lhs += [hid[n, pair(g)].reshape(32, ff) for n in ((R - s) % R, s)]
            to_partner(g, s).wait_recv()
        lhs = jnp.concatenate(lhs, axis=0)
        for t in range(half // C):
            at = pl.ds(t * C, C)
            p = jnp.dot(lhs, wdn[core, :, at], preferred_element_type=F32)
            for i, (g, s) in enumerate(chunks):
                mine = p[64 * i : 64 * i + 64].reshape(2, 2, 16, C)
                prx[g, s, :, :, :, at] = (mine + prx[g, s, :, :, :, at].astype(F32)).astype(BF16)

    def in_pairs(lo, hi, body):
        count = jnp.maximum(hi - lo, 0)

        def two(i, c):
            body([lo + 2 * i, lo + 2 * i + 1])
            return c

        lax.fori_loop(0, count // 2, two, 0)

        @when(count % 2 == 1)
        def _():
            body([hi - 1])

    whole_z = pl.ds(0, half)
    lows_z, highs_z = pl.ds(0, cut), pl.ds(cut, half - cut)

    halves_z = (lows_z, highs_z)

    def ring_first(d, g):
        cols = halves_z[d]
        return remote(
            prx.at[g, H, d, :, :, cols], ring.at[d, H - 1, pair(g), :, cols],
            sr.at[d, H - 1, g, d], rr.at[d, H - 1, g, d], b_to[d],
        )

    def ring_r(d, s, g, h):
        cols = halves_z[h]
        return remote(
            ring.at[d, s, pair(g), :, cols], ring.at[d, s - 1, pair(g), :, cols],
            sr.at[d, s - 1, g, h], rr.at[d, s - 1, g, h], b_to[d],
        )

    def arrived(d, s, g, h):
        here = ring.at[d, s, pair(g), :, halves_z[h]]
        remote(here, here, sr.at[d, s, g, h], rr.at[d, s, g, h], b_to[d]).wait_recv()

    def z_send(j, to):
        return remote(z_out.at[j], z_in.at[j], sz.at[j], rz.at[j], device(to % R, b))

    def sum_step(k, g):
        s = 2 * H + 1 - k + g

        @when(s == H)
        def _():
            for d in range(2):
                ring_first(d, g).start()

        @when((s >= 1) & (s < H))
        def _():
            for h in range(2):
                for d in range(2):
                    cols = halves_z[h]
                    if h == d:
                        arrived(d, s, g, h)
                    else:
                        @when(s < H - 1)
                        def _(d=d, h=h):
                            arrived(d, s, g, h)

                    ring[d, s, pair(g), :, cols] = (
                        ring[d, s, pair(g), :, cols].astype(F32) + prx[g, s, d, :, :, cols].astype(F32)
                    ).astype(BF16)
                    ring_r(d, s, g, h).start()

    def last_sum(g):
        for h in range(2):
            for d in range(2):
                arrived(d, 0, g, h)

        def part_of(i):
            v = ring[0, 0, 2 * g + i].astype(F32) + ring[1, 0, 2 * g + i].astype(F32)
            v = v + prx[g, 0, 0, i].astype(F32)
            z_out[2 * g + i] = v.astype(BF16)
            return v

        part_of(1)

        @when(g >= 2)
        def _():
            z_send(2 * g + 1, a + 2).start()

        near = part_of(0)

        @when(g >= 2)
        def _():
            z_send(2 * g, a + R - 2).start()

        @when(g == 0)
        def _():
            fin[...] = near

    def pass_on(held, far, step):
        z_send(far, a + 2).wait_recv()
        z_out[held] = (z_out[held].astype(F32) + z_in[far].astype(F32)).astype(BF16)
        z_send(held, a + step).start()

    def over_groups(body):
        lax.fori_loop(0, H, lambda g, c: (body(g), c)[1], 0)

    def stage(k, c):
        over_groups(lambda g: gather_step(k, g))
        over_groups(lambda i: sum_step(k, H - 1 - i))

        @when(k == 0)
        def _():
            for w in weights:
                w.wait()

        arrivals(k, own_arrivals)
        arrivals(k, par_arrivals)
        new = k - H

        @when((new >= 0) & (new < H))
        def _():
            def near(n, cc):
                activate(n, new)
                return cc

            def rest(g, cc):
                activate(new, g)
                activate(R - 1 - new, g)
                return cc

            lax.fori_loop(new, R - new, near, 0)
            lax.fori_loop(new + 1, H, rest, 0)
            partner_chunks([(new, H), (new, H - 1)])

        in_pairs(
            jnp.maximum(new - H + 1, 0), jnp.minimum(new, H),
            lambda gs: partner_chunks([(g, H - 1 - new + g) for g in gs]),
        )
        in_pairs(
            jnp.maximum(new - H, 0), jnp.minimum(new + 1, H),
            lambda gs: own_chunks([(g, H - new + g) for g in gs]),
        )

        @when(k >= 2 * H + 1)
        def _():
            last_sum(k - (2 * H + 1))

        return c

    lax.fori_loop(0, 3 * H + 1, stage, 0)
    bias_out[...] = bias_ref[...] + 2.0 / math.sqrt(average) * (average - loads[:, pl.ds(0, experts)])

    swap.wait_send()

    def drain_g(g, c):
        down(g).wait_send()

        @when(g < H - 1)
        def _():
            up(g).wait_send()

        def per_s(s, cc):
            @when(s < H - 1)
            def _():
                for d in range(2):
                    ring_x(d, s, g, whole).wait_send()

            @when(s == H - 1)
            def _():
                ring_x(0, H - 1, g, lows).wait_send()
                ring_x(1, H - 1, g, highs).wait_send()
                for d in range(2):
                    ring_first(d, g).wait_send()

            @when(s < H - 1)
            def _():
                for d in range(2):
                    for h in range(2):
                        ring_r(d, s + 1, g, h).wait_send()

            return cc

        lax.fori_loop(0, H, per_s, 0)

        def per_n(n, cc):
            across(n, g).wait_send()
            return cc

        lax.fori_loop(0, R, per_n, 0)

        def per_p(s, cc):
            to_partner(g, s).wait_send()
            return cc

        lax.fori_loop(0, H + 1, per_p, 0)
        return c

    lax.fori_loop(0, H, drain_g, 0)

    pass_on(1, 5, 1)
    pass_on(3, 7, 2)
    pass_on(2, 6, R - 1)
    total = fin[...]
    for j in (4, 1, 2, 3):
        z_send(j, a + 2).wait_recv()
        total = total + z_in[j].astype(F32)
    f_out[...] = jnp.where(first, total[8:], total[:8])
    kept = jnp.where(first, total[:8], total[8:])
    last = remote(f_out, f_in, sf.at[0], sf.at[1], partner)
    last.start()
    row = lax.broadcasted_iota(jnp.int32, (8, half), 0)

    def place(v):
        v = v.astype(BF16).astype(F32)
        placed = jnp.zeros((8, half), F32)
        for t in range(8):
            placed = jnp.where(row == home[t], jnp.broadcast_to(v[t : t + 1], (8, half)), placed)
        return placed

    kept = place(kept)

    for j in range(1, R):
        z_send(j, a + 2).wait_send()
    last.wait()
    other = place(f_in[...])
    out[:, pl.ds(0, half)] = jnp.where(first, kept, other).astype(BF16)
    out[:, pl.ds(half, half)] = jnp.where(first, other, kept).astype(BF16)


def per_device(tokens, experts, gate_fixed, home_slot, bias, w_gate, w_up, w_down):
    tok_rows, width = tokens.shape
    count = bias.shape[0]
    devices = lax.axis_size("ep")
    shards = devices // count
    side = math.isqrt(devices // 2)
    R, H = side, side // 2
    half = width // 2
    ff = w_gate.shape[1]
    average = tok_rows * devices * experts.shape[1] / count
    vmem = pl.BlockSpec(memory_space=pltpu.VMEM)
    smem = pl.BlockSpec(memory_space=pltpu.SMEM)
    anywhere = pl.BlockSpec(memory_space=pl.ANY)
    dma = pltpu.SemaphoreType.DMA
    out, bias_next = pl.pallas_call(
        functools.partial(kernel, (side, count, shards, average)),
        out_shape=(
            jax.ShapeDtypeStruct((tok_rows, width), BF16),
            jax.ShapeDtypeStruct((1, count), F32),
        ),
        in_specs=[smem, vmem, vmem, vmem, vmem, anywhere, anywhere, anywhere],
        out_specs=(vmem, vmem),
        scratch_shapes=[
            pltpu.VMEM((tok_rows, half + 128), BF16),
            pltpu.VMEM((tok_rows, half + 128), BF16),
            pltpu.VMEM((R, R, 16, half + 128), BF16),
            pltpu.VMEM((R, R, 16, half + 128), BF16),
            pltpu.VMEM((2, half, 2 * ff), BF16),
            pltpu.VMEM((2, ff, half), BF16),
            pltpu.VMEM((R, R, 16, 2 * ff), F32),
            pltpu.VMEM((R, R, 16, 2 * ff), F32),
            pltpu.VMEM((R, R, 16, ff), BF16),
            pltpu.VMEM((H, H + 1, 2, 2, 16, half), BF16),
            pltpu.VMEM((H, H + 1, 2, 2, 16, half), BF16),
            pltpu.VMEM((2, H, R, 16, half), BF16),
            pltpu.VMEM((R, 16, half), BF16),
            pltpu.VMEM((R, 16, half), BF16),
            pltpu.VMEM((16, half), F32),
            pltpu.VMEM((tok_rows, half), F32),
            pltpu.VMEM((tok_rows, half), F32),
            pltpu.VMEM((1, 128), F32),
            dma((6,)),
            dma((2,)),
            dma((2, H)),
            dma((2, H)),
            dma((2, H, H)),
            dma((2, H, H)),
            dma((R, H)),
            dma((R, H)),
            dma((H, H + 1)),
            dma((H, H + 1)),
            dma((2, H, H, 2)),
            dma((2, H, H, 2)),
            dma((R,)),
            dma((R,)),
            dma((2,)),
        ],
        compiler_params=pltpu.CompilerParams(
            collective_id=0, has_side_effects=True, vmem_limit_bytes=67_000_000
        ),
        name="routed_experts",
    )(home_slot, tokens, experts, gate_fixed, bias.reshape(1, count), w_gate, w_up, w_down)
    return (out, bias_next.reshape(count))


def solution(mesh):
    placed = (
        P(("groups", "ep"), None),
        P(("groups", "ep"), None),
        P(("groups", "ep"), None),
        P(("groups", "ep")),
        P(),
        P(None, "ep"),
        P(None, "ep"),
        P("ep", None),
    )
    return jax.shard_map(
        per_device,
        mesh=mesh,
        in_specs=placed,
        out_specs=(P(("groups", "ep"), None), P("groups")),
        check_vma=False,
    )
```

```python
import functools
import math

import jax
import jax.numpy as jnp
from jax import lax
from jax.experimental import pallas as pl
from jax.experimental.pallas import tpu as pltpu
from jax.sharding import PartitionSpec as P

ROUTED_SCALE = 2.5
F32 = jnp.float32
BF16 = jnp.bfloat16


def when(cond):
    return pl.when(cond)


def kernel(
    dims, home, tok, exp_ref, gate_ref, bias_ref, wg, wu, wd,
    out, bias_out,
    xs, xr, x_own, x_par, wgu, wdn, acc_own, acc_par, hid, pst, prx, ring, z_out, z_in, fin, f_out, f_in, loads,
    w_sem, x_sem, s1, r1, s2, r2, sd, rd, sp, rp, sr, rr, sz, rz, sf,
):
    side, experts, shards, average = dims
    R, H = side, side // 2
    assert R == 8
    top = exp_ref.shape[1]
    half = tok.shape[1] // 2
    wide = half + 128
    cut = (half // 2) // 128 * 128
    ff = wg.shape[1]
    me = lax.axis_index("ep")
    core = me % 2
    x = (me // 2) % side
    y = me // (2 * side)
    a = y + core * (x - y)
    b = x + core * (y - x)

    def device(aa, bb):
        yy = aa + core * (bb - aa)
        xx = bb + core * (aa - bb)
        return {"ep": (yy * side + xx) * 2 + core}

    a_next, a_prev = device((a + 1) % R, b), device((a + R - 1) % R, b)
    b_next, b_prev = device(a, (b + 1) % R), device(a, (b + R - 1) % R)
    partner = {"ep": me + 1 - 2 * core}
    b_to = (b_next, b_prev)

    def remote(src, dst, send, recv, to):
        return pltpu.make_async_remote_copy(
            src_ref=src, dst_ref=dst, send_sem=send, recv_sem=recv,
            device_id=to, device_id_type=pl.DeviceIdType.MESH,
        )

    weights = []
    for h in range(2):
        rows = pl.ds(h * half, half)
        weights.append(pltpu.make_async_copy(wg.at[rows, :], wgu.at[h, :, pl.ds(0, ff)], w_sem.at[3 * h]))
        weights.append(pltpu.make_async_copy(wu.at[rows, :], wgu.at[h, :, pl.ds(ff, ff)], w_sem.at[3 * h + 1]))
        weights.append(pltpu.make_async_copy(wd.at[:, rows], wdn.at[h], w_sem.at[3 * h + 2]))
    for w in weights:
        w.start()

    barrier = pltpu.get_barrier_semaphore()
    for to in [partner, b_next, b_prev] + [device((a + i) % R, b) for i in (1, 2, R - 2, R - 1)]:
        pl.semaphore_signal(barrier, inc=1, device_id=to, device_id_type=pl.DeviceIdType.MESH)

    fixed = gate_ref[...].astype(F32)
    share = ROUTED_SCALE * fixed / jnp.sum(fixed, axis=1, keepdims=True)
    ids = exp_ref[...]
    lane = lax.broadcasted_iota(jnp.int32, (tok.shape[0], 128), 1)
    expert_of = lane % experts
    hit = jnp.zeros(lane.shape, F32)
    val = jnp.zeros(lane.shape, F32)
    for k in range(top):
        same = expert_of == ids[:, k : k + 1]
        hit = hit + jnp.where(same, 1.0, 0.0)
        val = val + jnp.where(same, share[:, k : k + 1], 0.0)
    high = val.astype(BF16).astype(F32)
    rest = val - high
    mid = rest.astype(BF16).astype(F32)
    low = rest - mid
    part = lane // experts
    meta = jnp.where(part == 0, hit, 0.0)
    meta = jnp.where(part == 1, high, meta)
    meta = jnp.where(part == 2, mid, meta)
    meta = jnp.where(part == 3, low, meta)
    first = core == 0

    def place(v):
        row = lax.broadcasted_iota(jnp.int32, v.shape, 0)
        placed = jnp.zeros(v.shape, F32)
        for t in range(v.shape[0]):
            placed = jnp.where(row == home[t], jnp.broadcast_to(v[t : t + 1], v.shape), placed)
        return placed

    meta = place(meta)
    lo_half = place(tok[:, pl.ds(0, half)].astype(F32))
    hi_half = place(tok[:, pl.ds(half, half)].astype(F32))
    mine = jnp.where(first, lo_half, hi_half)
    xs[:, pl.ds(0, half)] = jnp.where(first, hi_half, lo_half).astype(BF16)
    xs[:, pl.ds(half, 128)] = meta.astype(BF16)

    pl.semaphore_wait(barrier, 7)
    swap = remote(xs, xr, x_sem.at[0], x_sem.at[1], partner)
    swap.start()
    swap.wait_recv()
    got = xr[...].astype(F32)
    x_own[0, 0, :, pl.ds(0, half)] = jnp.where(
        first,
        jnp.concatenate([mine, got[:, :half]], axis=0),
        jnp.concatenate([got[:, :half], mine], axis=0),
    ).astype(BF16)
    x_own[0, 0, :, pl.ds(half, 128)] = jnp.where(
        first,
        jnp.concatenate([meta, got[:, half:]], axis=0),
        jnp.concatenate([got[:, half:], meta], axis=0),
    ).astype(BF16)

    def down(g):
        src = jnp.maximum(2 * g - 1, 0) if not isinstance(g, int) else max(2 * g - 1, 0)
        return remote(x_own.at[0, src], x_own.at[0, 2 * g + 1], s1.at[1, g], r1.at[1, g], a_prev)

    def up(g):
        return remote(x_own.at[0, 2 * g], x_own.at[0, 2 * g + 2], s1.at[0, g], r1.at[0, g], a_next)

    down(0).start()
    up(0).start()

    def clear(j, c):
        ring[0, H - 1, j, :, pl.ds(cut, half - cut)] = jnp.zeros((16, half - cut), BF16)
        ring[1, H - 1, j, :, pl.ds(0, cut)] = jnp.zeros((16, cut), BF16)
        return c

    lax.fori_loop(0, R, clear, 0)

    whole = pl.ds(0, wide)
    lows, highs = pl.ds(0, cut), pl.ds(cut, wide - cut)

    def ring_x(d, s, g, cols):
        n = s if d == 0 else (R - s) % R
        to = s + 1 if d == 0 else R - s - 1
        return remote(
            x_own.at[n, pl.ds(2 * g, 2), :, cols], x_own.at[to, pl.ds(2 * g, 2), :, cols],
            s2.at[d, s, g], r2.at[d, s, g], b_to[d],
        )

    def across(n, g):
        return remote(
            x_own.at[n, pl.ds(2 * g, 2)], x_par.at[n, pl.ds(2 * g, 2)], sd.at[n, g], rd.at[n, g], partner
        )

    def gather_step(k, g):
        s = k - g

        @when(s == 0)
        def _():
            down(g).wait_recv()

            @when(g < H - 1)
            def _():
                down(g + 1).start()
                up(g).wait_recv()

            @when(g < H - 2)
            def _():
                up(g + 1).start()

        @when((s >= 1) & (s < H))
        def _():
            for d in range(2):
                ring_x(d, s - 1, g, whole).wait_recv()

        @when(s == H)
        def _():
            ring_x(0, H - 1, g, lows).wait_recv()
            ring_x(1, H - 1, g, highs).wait_recv()

        @when((s >= 0) & (s < H - 1))
        def _():
            for d in range(2):
                ring_x(d, s, g, whole).start()

        @when(s == H - 1)
        def _():
            ring_x(0, H - 1, g, lows).start()
            ring_x(1, H - 1, g, highs).start()

        @when((s >= 0) & (s <= H))
        def _():
            across(s, g).start()

        @when((s >= 1) & (s < H))
        def _():
            across(R - s, g).start()

    def slot_of(n):
        return jnp.where(n < H, 2 * n, 2 * R - 1 - 2 * n)

    def pair(g):
        return pl.ds(2 * g, 2)

    def gate_up(x_ref, acc_ref, w, chunks):
        at = [(n, pair(g)) for g, s in chunks for n in (s, (R - s) % R)]
        rows = jnp.concatenate(
            [x_ref[n, p, :, pl.ds(0, half)].reshape(32, half) for n, p in at], axis=0
        )
        prod = jnp.dot(rows, wgu[w], preferred_element_type=F32)
        for i, (n, p) in enumerate(at):
            acc_ref[n, p] = prod[32 * i : 32 * i + 32].reshape(2, 16, 2 * ff)

    def arrivals(k, body):
        def unit(u, c):
            s0 = k - 2 * u
            v0 = (s0 >= 0) & (s0 <= H)
            v1 = (s0 >= 1) & (s0 <= H + 1)

            @when(v0 | v1)
            def _():
                g0 = 2 * u + jnp.where(v0, 0, 1)
                g1 = 2 * u + jnp.where(v1, 1, 0)
                body(v0, v1, [(g0, k - g0), (g1, k - g1)])

            return c

        lax.fori_loop(0, H // 2, unit, 0)

    def own_arrivals(v0, v1, chunks):
        gate_up(x_own, acc_own, core, chunks)

    def par_arrivals(v0, v1, chunks):
        for v, (g, s) in zip((v0, v1), chunks):
            @when(v)
            def _(g=g, s=s):
                across(s, g).wait_recv()

                @when((s >= 1) & (s < H))
                def _():
                    across(R - s, g).wait_recv()

        gate_up(x_par, acc_par, 1 - core, chunks)

    my_expert = me // shards
    lane = lax.broadcasted_iota(jnp.int32, (32, 128), 1)
    gated = (lane % experts == my_expert) & (lane >= experts) & (lane < 4 * experts)

    def activate(n, g):
        m = x_own[n, pair(g), :, pl.ds(half, 128)].reshape(32, 128).astype(F32)
        gate = jnp.sum(jnp.where(gated, m, 0.0), axis=1, keepdims=True)
        j = slot_of(n)
        both = acc_own[n, pair(g)].reshape(32, 2 * ff) + jnp.concatenate(
            [acc_par[g, j], acc_par[R - 1 - g, j]], axis=0
        )
        v = both[:, :ff]
        h = v / (1.0 + jnp.exp(-v)) * both[:, ff:] * gate
        hid[n, pair(g)] = h.astype(BF16).reshape(2, 16, ff)
        loads[...] += jnp.sum(m, axis=0, keepdims=True)

    loads[...] = jnp.zeros((1, 128), F32)

    C = 512 if half % 512 == 0 else 128

    def to_partner(g, s):
        return remote(pst.at[g, s], prx.at[g, s], sp.at[g, s], rp.at[g, s], partner)

    def partner_chunks(chunks):
        lhs = []
        for g, s in chunks:
            j1, j2 = slot_of((R - s) % R), slot_of(s)
            lhs += [hid[g, j1], hid[R - 1 - g, j1], hid[g, j2], hid[R - 1 - g, j2]]
        lhs = jnp.concatenate(lhs, axis=0)
        for t in range(half // C):
            at = pl.ds(t * C, C)
            p = jnp.dot(lhs, wdn[1 - core, :, at], preferred_element_type=F32).astype(BF16)
            for i, (g, s) in enumerate(chunks):
                pst[g, s, :, :, :, at] = p[64 * i : 64 * i + 64].reshape(2, 2, 16, C)
        for g, s in chunks:
            to_partner(g, s).start()

    def own_chunks(chunks):
        lhs = []
        for g, s in chunks:
            lhs += [hid[n, pair(g)].reshape(32, ff) for n in ((R - s) % R, s)]
            to_partner(g, s).wait_recv()
        lhs = jnp.concatenate(lhs, axis=0)
        for t in range(half // C):
            at = pl.ds(t * C, C)
            p = jnp.dot(lhs, wdn[core, :, at], preferred_element_type=F32)
            for i, (g, s) in enumerate(chunks):
                mine = p[64 * i : 64 * i + 64].reshape(2, 2, 16, C)
                prx[g, s, :, :, :, at] = (mine + prx[g, s, :, :, :, at].astype(F32)).astype(BF16)

    def in_pairs(lo, hi, body):
        count = jnp.maximum(hi - lo, 0)

        def two(i, c):
            body([lo + 2 * i, lo + 2 * i + 1])
            return c

        lax.fori_loop(0, count // 2, two, 0)

        @when(count % 2 == 1)
        def _():
            body([hi - 1])

    whole_z = pl.ds(0, half)
    lows_z, highs_z = pl.ds(0, cut), pl.ds(cut, half - cut)

    halves_z = (lows_z, highs_z)

    def ring_first(d, g):
        cols = halves_z[d]
        return remote(
            prx.at[g, H, d, :, :, cols], ring.at[d, H - 1, pair(g), :, cols],
            sr.at[d, H - 1, g], rr.at[d, H - 1, g], b_to[d],
        )

    def ring_r(d, s, g):
        return remote(
            ring.at[d, s, pair(g)], ring.at[d, s - 1, pair(g)],
            sr.at[d, s - 1, g], rr.at[d, s - 1, g], b_to[d],
        )

    def z_send(j, to):
        return remote(z_out.at[j], z_in.at[j], sz.at[j], rz.at[j], device(to % R, b))

    def sum_step(k, g):
        s = 2 * H + 1 - k + g

        @when(s == H)
        def _():
            for d in range(2):
                ring_first(d, g).start()

        @when((s >= 1) & (s < H))
        def _():
            for d in range(2):
                @when(s == H - 1)
                def _(d=d):
                    ring_first(d, g).wait_recv()

                @when(s < H - 1)
                def _(d=d):
                    ring_r(d, s + 1, g).wait_recv()

                ring[d, s, pair(g)] = (
                    ring[d, s, pair(g)].astype(F32) + prx[g, s, d].astype(F32)
                ).astype(BF16)
                ring_r(d, s, g).start()

    def last_sum(g):
        for d in range(2):
            ring_r(d, 1, g).wait_recv()

        def part_of(i):
            v = ring[0, 0, 2 * g + i].astype(F32) + ring[1, 0, 2 * g + i].astype(F32)
            v = v + prx[g, 0, 0, i].astype(F32)
            z_out[2 * g + i] = v.astype(BF16)
            return v

        part_of(1)

        @when(g >= 2)
        def _():
            z_send(2 * g + 1, a + 2).start()

        near = part_of(0)

        @when(g >= 2)
        def _():
            z_send(2 * g, a + R - 2).start()

        @when(g == 0)
        def _():
            fin[...] = near

    def pass_on(held, far, step):
        z_send(far, a + 2).wait_recv()
        z_out[held] = (z_out[held].astype(F32) + z_in[far].astype(F32)).astype(BF16)
        z_send(held, a + step).start()

    def over_groups(body):
        lax.fori_loop(0, H, lambda g, c: (body(g), c)[1], 0)

    def stage(k, c):
        over_groups(lambda g: gather_step(k, g))
        over_groups(lambda i: sum_step(k, H - 1 - i))

        @when(k == 0)
        def _():
            for w in weights:
                w.wait()

        arrivals(k, own_arrivals)
        arrivals(k, par_arrivals)
        new = k - H

        @when((new >= 0) & (new < H))
        def _():
            def near(n, cc):
                activate(n, new)
                return cc

            def rest(g, cc):
                activate(new, g)
                activate(R - 1 - new, g)
                return cc

            lax.fori_loop(new, R - new, near, 0)
            lax.fori_loop(new + 1, H, rest, 0)
            partner_chunks([(new, H), (new, H - 1)])

        in_pairs(
            jnp.maximum(new - H + 1, 0), jnp.minimum(new, H),
            lambda gs: partner_chunks([(g, H - 1 - new + g) for g in gs]),
        )
        in_pairs(
            jnp.maximum(new - H, 0), jnp.minimum(new + 1, H),
            lambda gs: own_chunks([(g, H - new + g) for g in gs]),
        )

        @when(k >= 2 * H + 1)
        def _():
            last_sum(k - (2 * H + 1))

        return c

    lax.fori_loop(0, 3 * H + 1, stage, 0)
    bias_out[...] = bias_ref[...] + 2.0 / math.sqrt(average) * (average - loads[:, pl.ds(0, experts)])

    swap.wait_send()

    def drain_g(g, c):
        down(g).wait_send()

        @when(g < H - 1)
        def _():
            up(g).wait_send()

        def per_s(s, cc):
            @when(s < H - 1)
            def _():
                for d in range(2):
                    ring_x(d, s, g, whole).wait_send()

            @when(s == H - 1)
            def _():
                ring_x(0, H - 1, g, lows).wait_send()
                ring_x(1, H - 1, g, highs).wait_send()
                for d in range(2):
                    ring_first(d, g).wait_send()

            @when(s < H - 1)
            def _():
                for d in range(2):
                    ring_r(d, s + 1, g).wait_send()

            return cc

        lax.fori_loop(0, H, per_s, 0)

        def per_n(n, cc):
            across(n, g).wait_send()
            return cc

        lax.fori_loop(0, R, per_n, 0)

        def per_p(s, cc):
            to_partner(g, s).wait_send()
            return cc

        lax.fori_loop(0, H + 1, per_p, 0)
        return c

    lax.fori_loop(0, H, drain_g, 0)

    pass_on(1, 5, 1)
    pass_on(3, 7, 2)
    pass_on(2, 6, R - 1)
    total = fin[...]
    for j in (4, 1, 2, 3):
        z_send(j, a + 2).wait_recv()
        total = total + z_in[j].astype(F32)
    f_out[...] = jnp.where(first, total[8:], total[:8]).astype(BF16)
    kept = jnp.where(first, total[:8], total[8:])
    last = remote(f_out, f_in, sf.at[0], sf.at[1], partner)
    last.start()
    for j in range(1, R):
        z_send(j, a + 2).wait_send()
    last.wait()
    other = f_in[...].astype(F32)
    out[:, pl.ds(0, half)] = jnp.where(first, kept, other).astype(BF16)
    out[:, pl.ds(half, half)] = jnp.where(first, other, kept).astype(BF16)


def per_device(tokens, experts, gate_fixed, home_slot, bias, w_gate, w_up, w_down):
    tok_rows, width = tokens.shape
    count = bias.shape[0]
    devices = lax.axis_size("ep")
    shards = devices // count
    side = math.isqrt(devices // 2)
    R, H = side, side // 2
    half = width // 2
    ff = w_gate.shape[1]
    average = tok_rows * devices * experts.shape[1] / count
    vmem = pl.BlockSpec(memory_space=pltpu.VMEM)
    smem = pl.BlockSpec(memory_space=pltpu.SMEM)
    anywhere = pl.BlockSpec(memory_space=pl.ANY)
    dma = pltpu.SemaphoreType.DMA
    out, bias_next = pl.pallas_call(
        functools.partial(kernel, (side, count, shards, average)),
        out_shape=(
            jax.ShapeDtypeStruct((tok_rows, width), BF16),
            jax.ShapeDtypeStruct((1, count), F32),
        ),
        in_specs=[smem, vmem, vmem, vmem, vmem, anywhere, anywhere, anywhere],
        out_specs=(vmem, vmem),
        scratch_shapes=[
            pltpu.VMEM((tok_rows, half + 128), BF16),
            pltpu.VMEM((tok_rows, half + 128), BF16),
            pltpu.VMEM((R, R, 16, half + 128), BF16),
            pltpu.VMEM((R, R, 16, half + 128), BF16),
            pltpu.VMEM((2, half, 2 * ff), BF16),
            pltpu.VMEM((2, ff, half), BF16),
            pltpu.VMEM((R, R, 16, 2 * ff), F32),
            pltpu.VMEM((R, R, 16, 2 * ff), F32),
            pltpu.VMEM((R, R, 16, ff), BF16),
            pltpu.VMEM((H, H + 1, 2, 2, 16, half), BF16),
            pltpu.VMEM((H, H + 1, 2, 2, 16, half), BF16),
            pltpu.VMEM((2, H, R, 16, half), BF16),
            pltpu.VMEM((R, 16, half), BF16),
            pltpu.VMEM((R, 16, half), BF16),
            pltpu.VMEM((16, half), F32),
            pltpu.VMEM((tok_rows, half), BF16),
            pltpu.VMEM((tok_rows, half), BF16),
            pltpu.VMEM((1, 128), F32),
            dma((6,)),
            dma((2,)),
            dma((2, H)),
            dma((2, H)),
            dma((2, H, H)),
            dma((2, H, H)),
            dma((R, H)),
            dma((R, H)),
            dma((H, H + 1)),
            dma((H, H + 1)),
            dma((2, H, H)),
            dma((2, H, H)),
            dma((R,)),
            dma((R,)),
            dma((2,)),
        ],
        compiler_params=pltpu.CompilerParams(
            collective_id=0, has_side_effects=True, vmem_limit_bytes=67_000_000
        ),
        name="routed_experts",
    )(home_slot, tokens, experts, gate_fixed, bias.reshape(1, count), w_gate, w_up, w_down)
    return (out, bias_next.reshape(count))


def solution(mesh):
    placed = (
        P(("groups", "ep"), None),
        P(("groups", "ep"), None),
        P(("groups", "ep"), None),
        P(("groups", "ep")),
        P(),
        P(None, "ep"),
        P(None, "ep"),
        P("ep", None),
    )
    return jax.shard_map(
        per_device,
        mesh=mesh,
        in_specs=placed,
        out_specs=(P(("groups", "ep"), None), P("groups")),
        check_vma=False,
    )
```
